512 devices in a mesh: hot: 16 (over z, core), cold: 32 (over x, y).
Axes of the slice: x: 4, y: 8, z: 8, core: 2. Of those that a mesh axis runs over, the one named last changes fastest.
Arguments:
- tokens: bfloat16 [512, 8192], P('cold', 'hot'), may hold values from -6 to 6
- hot_gate: bfloat16 [8192, 4096], P('hot', 'cold'), may hold values from -0.0625 to 0.0625
- hot_up: bfloat16 [8192, 4096], P('hot', 'cold'), may hold values from -0.0625 to 0.0625
- hot_down: bfloat16 [4096, 8192], P('cold', 'hot'), may hold values from -0.0625 to 0.0625
- cold_gate: bfloat16 [8192, 24576], P('hot', 'cold'), may hold values from -0.0625 to 0.0625
- cold_up: bfloat16 [8192, 24576], P('hot', 'cold'), may hold values from -0.0625 to 0.0625
- cold_down: bfloat16 [24576, 8192], P('cold', 'hot'), may hold values from -0.0625 to 0.0625
- hot_ids: int32 [32], replicated, may hold values from 0 to 223, as said below
- cold_ids: int32 [192], replicated, may hold values from 0 to 223, as said below
- block_mask: int32 [512, 224], replicated, may hold values from 0 to 1, as said below
Outputs:
- mixed: bfloat16 [512, 8192], P('cold', 'hot')
The draws below stay inside these ranges and needn't reach their ends.
Inputs may be any that keep to these rules, and one draw needn't show every extreme that they name: hot_ids and cold_ids together name every block number from 0 to 223 once. `cold_ids`: cold slot s lies with index s // 6 of cold. `block_mask`: among the 16 tokens of one index of cold, at most 8 have a 1 in a cold slot of one given index of cold; in every draw some index of cold gets exactly 8 such tokens from every index of cold.
All inputs are finite; a program needn't handle non-finite values.
Results may differ from the reference program's by a relative error of at most 0.0049.
Values may be sent and summed in bfloat16 or wider, within the bound.
A program may use at most 64 MiB of HBM per device.

```python
import jax
import jax.numpy as jnp
from jax import lax

D = 8192
BLOCK = 128
COLD_DEV = 6
TOK_DEV = 16
CAP = 8
TOKENS = 512
HB = 32
CB = 192
NB = 224
FF = 28672
N_COLD = 32


def rank_tokens(rank_key):
    return jax.random.permutation(rank_key, TOK_DEV).astype(jnp.int32)


def routing_tables(key):
    folded = jax.random.fold_in(key, 41)
    subkeys = jax.random.split(folded, 11)
    middle = (jax.random.permutation(subkeys[0], NB - 2) + 1).astype(jnp.int32)
    hot_list = jnp.concatenate([middle[:HB - 1], jnp.zeros((1,), jnp.int32)])
    cold_list = jnp.concatenate([middle[HB - 1:], jnp.full((1,), NB - 1, jnp.int32)])
    hot_ids = jnp.take(hot_list, jax.random.permutation(subkeys[9], HB).astype(jnp.int32))
    cold_ids = jnp.take(cold_list, jax.random.permutation(subkeys[10], CB).astype(jnp.int32))
    group_total = CB // COLD_DEV
    sources = TOKENS // TOK_DEV
    group_level = jax.random.randint(subkeys[1], (group_total,), 1, 5)
    busy_group = jax.random.randint(subkeys[2], (), 0, group_total)
    ceiling = group_level * CAP // 4
    hit_count = jax.random.randint(subkeys[3], (sources, group_total), 0, ceiling[None, :] + 1)
    hit_count = jnp.where(jnp.arange(group_total)[None, :] == busy_group, CAP, hit_count)
    rank_keys = jax.random.split(subkeys[4], sources * group_total)
    token_ranks = jax.vmap(rank_tokens)(rank_keys).reshape(sources, group_total, TOK_DEV)
    group_hit = token_ranks < hit_count[:, :, None]
    first_block = jax.random.randint(subkeys[5], (sources, group_total, TOK_DEV), 0, COLD_DEV)
    extra_blocks = jax.random.randint(subkeys[6], (sources, group_total, TOK_DEV, COLD_DEV), 0, 4) == 0
    chosen_blocks = (first_block[..., None] == jnp.arange(COLD_DEV)) | extra_blocks
    chosen_blocks = chosen_blocks & group_hit[..., None]
    cold_mask = jnp.transpose(chosen_blocks, (0, 2, 1, 3)).reshape(TOKENS, CB).astype(jnp.int32)
    hot_rate = jax.random.randint(subkeys[7], (HB,), 5, 10)
    hot_mask = (jax.random.randint(subkeys[8], (TOKENS, HB), 0, 10) < hot_rate[None, :]).astype(jnp.int32)
    block_mask = jnp.zeros((TOKENS, NB), jnp.int32)
    block_mask = block_mask.at[:, hot_ids].set(hot_mask)
    block_mask = block_mask.at[:, cold_ids].set(cold_mask)
    return (hot_ids, cold_ids, block_mask)


def draw_hot_ids(key, part):
    return routing_tables(key)[0]


def draw_cold_ids(key, part):
    return routing_tables(key)[1]


def draw_block_mask(key, part):
    return routing_tables(key)[2]


def steps_of(stream_key, dims, shards, low, high):
    gain, own = 1.0, jax.random.fold_in(stream_key, 6)
    for axis_at, parts in shards:
        heights = jnp.exp(jax.random.uniform(jax.random.fold_in(own, axis_at), (parts,), jnp.float32, low / len(shards), high / len(shards)))
        gain = gain * jnp.repeat(heights, dims[axis_at] // parts).reshape([-1 if axis == axis_at else 1 for axis in range(len(dims))])
    return gain


def scatter_about(own_key, shape, spread, bound, pieces=(), kind=jnp.bfloat16):
    result = spread * jax.random.normal(own_key, shape, jnp.float32)
    if pieces:
        result = result * steps_of(own_key, shape, pieces, -0.22, 0.18)
    return jnp.clip(result, -bound, bound).astype(kind)


def setup_inputs(seed: int = 0) -> dict:
    arg_keys = jax.random.split(jax.random.key(seed), 11)
    tokens = scatter_about(arg_keys[0], (TOKENS, D), 1.0, 6.0, ((0, 32), (1, 16)))
    hot_gate = scatter_about(arg_keys[1], (D, HB * BLOCK), D ** -0.5, 0.0625, ((0, 16), (1, 32)))
    hot_up = scatter_about(arg_keys[2], (D, HB * BLOCK), D ** -0.5, 0.0625, ((0, 16), (1, 32)))
    hot_down = scatter_about(arg_keys[3], (HB * BLOCK, D), (FF // 4) ** -0.5, 0.0625, ((0, 32), (1, 16)))
    cold_gate = scatter_about(arg_keys[4], (D, CB * BLOCK), D ** -0.5, 0.0625, ((0, 16), (1, 32)))
    cold_up = scatter_about(arg_keys[5], (D, CB * BLOCK), D ** -0.5, 0.0625, ((0, 16), (1, 32)))
    cold_down = scatter_about(arg_keys[6], (CB * BLOCK, D), (FF // 4) ** -0.5, 0.0625, ((0, 32), (1, 16)))
    hot_ids = draw_hot_ids(jax.random.fold_in(arg_keys[10], 71), 0)
    cold_ids = draw_cold_ids(jax.random.fold_in(arg_keys[10], 71), 0)
    block_mask = draw_block_mask(jax.random.fold_in(arg_keys[10], 71), 0)
    return dict(tokens=tokens, hot_gate=hot_gate, hot_up=hot_up, hot_down=hot_down, cold_gate=cold_gate, cold_up=cold_up, cold_down=cold_down, hot_ids=hot_ids, cold_ids=cold_ids, block_mask=block_mask)


def ranged_product(matrix_rows, weight):
    return jnp.dot(matrix_rows, weight, preferred_element_type=jnp.float32)


def reference(tokens, hot_gate, hot_up, hot_down, cold_gate, cold_up, cold_down, hot_ids, cold_ids, block_mask):
    hot_bits = jnp.take(block_mask, hot_ids, axis=1)
    cold_bits = jnp.take(block_mask, cold_ids, axis=1)
    hot_gates = ranged_product(tokens, hot_gate)
    hot_ups = ranged_product(tokens, hot_up)
    hot_scale = jnp.repeat(hot_bits.astype(jnp.float32), BLOCK, axis=1)
    hot_hidden = (jax.nn.silu(hot_gates) * hot_ups * hot_scale).astype(jnp.bfloat16)
    hot_out = jnp.dot(hot_hidden, hot_down, preferred_element_type=jnp.float32)
    padded_tokens = jnp.concatenate([tokens, jnp.zeros((1, D), tokens.dtype)], axis=0)
    span = COLD_DEV * BLOCK

    def add_group(running, group_index):
        group_bits = lax.dynamic_slice_in_dim(cold_bits, (group_index * COLD_DEV).astype(jnp.int32), COLD_DEV, 1)
        group_hit = jnp.max(group_bits, axis=1) > 0
        picked = jnp.nonzero(group_hit, size=N_COLD * CAP, fill_value=TOKENS)[0].astype(jnp.int32)
        padded_bits = jnp.concatenate([group_bits, jnp.zeros((1, COLD_DEV), group_bits.dtype)], axis=0)
        picked_rows = jnp.take(padded_tokens, picked, axis=0)
        picked_bits = jnp.take(padded_bits, picked, axis=0)
        first_col = (group_index * span).astype(jnp.int32)
        gate_part = lax.dynamic_slice_in_dim(cold_gate, first_col, span, 1)
        up_part = lax.dynamic_slice_in_dim(cold_up, first_col, span, 1)
        down_part = lax.dynamic_slice_in_dim(cold_down, first_col, span, 0)
        gate_sum = ranged_product(picked_rows, gate_part)
        up_sum = ranged_product(picked_rows, up_part)
        scale = jnp.repeat(picked_bits.astype(jnp.float32), BLOCK, axis=1)
        hidden = (jax.nn.silu(gate_sum) * up_sum * scale).astype(jnp.bfloat16)
        group_out = jnp.dot(hidden, down_part, preferred_element_type=jnp.float32)
        return running.at[picked].add(group_out), None

    initial = jnp.zeros((TOKENS + 1, D), jnp.float32)
    cold_out = lax.scan(add_group, initial, jnp.arange(N_COLD, dtype=jnp.int32))[0]
    return (hot_out + cold_out[:TOKENS]).astype(jnp.bfloat16)
```

```python
import jax
import jax.numpy as jnp
from jax import lax
from jax.experimental import pallas as pl
from jax.experimental.pallas import tpu as pltpu
from jax.sharding import PartitionSpec as P

BLOCK = 128
NX, NY, NZ = 4, 8, 8
STEPS = 4
CAP = 8
ROWS = 16
TOK = NX * ROWS
SLOTS = NX * CAP
COLD = 6
F32, BF16 = jnp.float32, jnp.bfloat16
ORDER = ((0, 2, 6, 4), (1, 7, 3, 5))
SEND_ORDER = (0, 1, 2, 7, 6, 3, 4, 5)
FAR_FIRST = (4, 3, 5, 2, 6, 1, 7)
MESH = pl.DeviceIdType.MESH


def dot(a, b):
    return jnp.dot(a, b, preferred_element_type=F32)


def kernel(
    tok, hot_gate, hot_up, hot_down, cold_gate, cold_up, cold_down, hot_ids, cold_ids, mask,
    out,
    tokv, xbuf, wcg, wcu, wh, wd, mord, ptab, pmat, mz, sbuf, sown, rbuf, hbuf, obuf, oown, dbuf, ebuf, fbuf,
    tok_sem, mask_sem, wl_sem, ws_sem, wr_sem,
    a1s, a1z, a1r, a2s, a2r, bs, br, cs, cr, d1s, d1r, d2s, d2z, d2r, d2zr,
):
    hot, cold = lax.axis_index("hot"), lax.axis_index("cold")
    z, k = lax.div(hot, 2), lax.rem(hot, 2)
    x, y = lax.div(cold, NY), lax.rem(cold, NY)
    feat = tok.shape[1]

    def dev(px, py, pz, pk):
        return {"hot": pz * 2 + pk, "cold": px * NY + py}

    def at_x(d):
        return lax.rem(x + (d % NX), NX)

    def at_y(d):
        return lax.rem(y + NY + d, NY)

    def at_z(d):
        return lax.rem(z + (d % NZ), NZ)

    def dy_of(s):
        return ORDER[0][s] + k * (ORDER[1][s] - ORDER[0][s])

    def remote(src, dst, send, recv, to):
        return pltpu.make_async_remote_copy(
            src_ref=src, dst_ref=dst, send_sem=send, recv_sem=recv, device_id=to, device_id_type=MESH
        )

    here = dev(x, y, z, k)
    sister = dev(x, y, z, 1 - k)
    cols = pl.ds(pl.multiple_of(k * feat, feat), feat)
    mine = pl.ds(pl.multiple_of(k * feat, feat), feat)

    barrier = pltpu.get_barrier_semaphore()

    def greet(to):
        pl.semaphore_signal(barrier, inc=1, device_id=to, device_id_type=MESH)

    for d in range(1, NY):
        greet(dev(x, at_y(d), z, 0))
        greet(dev(x, at_y(d), z, 1))
    for d in range(1, NX):
        greet(dev(at_x(d), y, z, k))
    for d in range(1, NZ):
        greet(dev(x, y, at_z(d), k))
    greet(sister)

    tok_load = pltpu.make_async_copy(tok, tokv, tok_sem)
    tok_load.start()
    for s in range(STEPS):
        for dx in range(NX):
            group = at_x(dx) * NY + at_y(dy_of(s))
            pltpu.make_async_copy(
                mask.at[pl.ds(pl.multiple_of(group * ROWS, ROWS), ROWS), :],
                mord.at[pl.ds(s * TOK + dx * ROWS, ROWS), :],
                mask_sem,
            ).start()
    pieces = (
        (cold_gate, wcg.at[mine, :]),
        (cold_up, wcu.at[mine, :]),
        (hot_gate, wh.at[mine, pl.ds(0, BLOCK)]),
        (hot_up, wh.at[mine, pl.ds(BLOCK, BLOCK)]),
        (cold_down, wd.at[pl.ds(0, COLD * BLOCK), cols]),
        (hot_down, wd.at[pl.ds(COLD * BLOCK, BLOCK), cols]),
    )
    local_w = [pltpu.make_async_copy(a, b, wl_sem.at[i]) for i, (a, b) in enumerate(pieces)]
    remote_w = [remote(a, b, ws_sem.at[i], wr_sem.at[i], sister) for i, (a, b) in enumerate(pieces)]
    for copy in local_w:
        copy.start()

    pltpu.make_async_copy(mord, mord, mask_sem).wait()
    bits = mord[...].astype(F32).astype(BF16)
    blocks = mord.shape[1]
    block_no = lax.broadcasted_iota(jnp.int32, (blocks, BLOCK), 0)
    cold_sel = jnp.zeros((blocks, BLOCK), F32)
    for j in range(COLD):
        cold_sel = cold_sel + jnp.where(block_no == cold_ids[cold * COLD + j], 1.0, 0.0)
    unit_id = jnp.where(z < COLD, cold_ids[cold * COLD + jnp.minimum(z, COLD - 1)], hot_ids[cold])
    unit_sel = jnp.where(block_no == unit_id, 1.0, 0.0)
    hit = jnp.minimum(dot(bits, cold_sel.astype(BF16)), 1.0)
    unit_bit = dot(bits, unit_sel.astype(BF16))
    total = STEPS * TOK
    row = lax.broadcasted_iota(jnp.int32, (total, total), 0)
    col = lax.broadcasted_iota(jnp.int32, (total, total), 1)
    earlier = (lax.div(row, ROWS) == lax.div(col, ROWS)) & (col < row)
    slot = dot(jnp.where(earlier, 1.0, 0.0).astype(BF16), hit.astype(BF16))
    row = lax.broadcasted_iota(jnp.int32, (total, BLOCK), 0)
    lane = lax.broadcasted_iota(jnp.int32, (total, BLOCK), 1)
    base = lax.rem(lax.div(row, ROWS), NX) * CAP
    chosen = jnp.where((slot + base.astype(F32) == lane.astype(F32)) & (hit > 0.5), 1.0, 0.0)
    for s in range(STEPS):
        step_rows = slice(s * TOK, (s + 1) * TOK)
        pick = chosen[step_rows]
        ptab[s] = pick.astype(BF16)
        turned = jnp.transpose(pick)[:SLOTS].astype(BF16)
        pmat[s] = turned
        tokens_bit = unit_bit[step_rows]
        slot_bit = dot(turned, tokens_bit.astype(BF16))
        half_bit = jnp.where(z == COLD, tokens_bit[:SLOTS], tokens_bit[SLOTS:])
        mz[s] = jnp.where(z < COLD, slot_bit, half_bit)

    tok_load.wait()
    pl.semaphore_wait(barrier, 2 * (NY - 1) + (NX - 1) + (NZ - 1) + 1)

    for dy in SEND_ORDER:
        core = dy % 2
        s = ORDER[core].index(dy)
        spot = xbuf.at[s, pl.ds(0, ROWS), cols]
        if dy:
            remote(tokv, spot, a1s, a1r.at[s], dev(x, at_y(-dy), z, core)).start()
        else:

            @pl.when(k == 0)
            def _():
                pltpu.make_async_copy(tok, xbuf.at[0, pl.ds(0, ROWS), pl.ds(0, feat)], a1r.at[0]).start()

            @pl.when(k == 1)
            def _():
                remote(
                    tokv, xbuf.at[0, pl.ds(0, ROWS), pl.ds(feat, feat)], a1z, a1r.at[0], sister
                ).start()

    for copy in remote_w:
        copy.start()

    for s in range(STEPS):
        head = xbuf.at[s, pl.ds(0, ROWS), :]
        remote(head, head, a2s.at[s], a1r.at[s], here).wait_recv()
        for dx in (2, 1, 3):
            remote(
                head, xbuf.at[s, pl.ds(dx * ROWS, ROWS), :], a2s.at[s], a2r.at[s], dev(at_x(-dx), y, z, k)
            ).start()

    for s in range(STEPS):
        rest = xbuf.at[s, pl.ds(ROWS, TOK - ROWS), :]
        remote(rest, rest, a2s.at[s], a2r.at[s], here).wait_recv()
        if s == 0:
            for i in range(4):
                local_w[i].wait()
                remote_w[i].wait_recv()
        rows = xbuf[s]
        picked = dot(pmat[s], rows).astype(BF16)
        gates, ups = dot(picked, wcg[...]), dot(picked, wcu[...])
        hots = dot(rows, wh[...])
        for j in range(NZ):
            if j < COLD:
                part = slice(j * BLOCK, (j + 1) * BLOCK)
                gate, up = gates[:, part], ups[:, part]
            else:
                part = slice((j - COLD) * SLOTS, (j - COLD + 1) * SLOTS)
                gate, up = hots[part, :BLOCK], hots[part, BLOCK:]
            sown[s, j, :, :BLOCK] = gate
            sown[s, j, :, BLOCK:] = up
            sbuf[s, j, :, :BLOCK] = gate.astype(BF16)
            sbuf[s, j, :, BLOCK:] = up.astype(BF16)
        for dz in FAR_FIRST:
            remote(
                sbuf.at[s, at_z(dz)], rbuf.at[s, dz - 1], bs.at[s], br.at[s], dev(x, y, at_z(dz), k)
            ).start()

    for s in range(STEPS):
        remote(rbuf.at[s], rbuf.at[s], bs.at[s], br.at[s], here).wait_recv()
        terms = sown[s, z]
        for i in range(NZ - 1):
            terms = terms + rbuf[s, i].astype(F32)
        gate, up = terms[:, :BLOCK], terms[:, BLOCK:]
        hidden = gate / (1.0 + jnp.exp(-gate)) * up * mz[s]
        hbuf[s, z] = hidden.astype(BF16)
        for dz in FAR_FIRST:
            remote(
                hbuf.at[s, z], hbuf.at[s, z], cs.at[s], cr.at[s], dev(x, y, at_z(dz), k)
            ).start()

    for s in range(STEPS):
        most = hbuf.at[s, pl.ds(0, NZ - 1)]
        remote(most, most, cs.at[s], cr.at[s], here).wait_recv()
        if s == 0:
            for i in (4, 5):
                local_w[i].wait()
                remote_w[i].wait_recv()
        colds = jnp.concatenate([hbuf[s, j] for j in range(COLD)], axis=1)
        spread = dot(ptab[s][:, :SLOTS], colds).astype(BF16)
        hots = jnp.concatenate([hbuf[s, COLD], hbuf[s, COLD + 1]], axis=0)
        result = dot(spread, wd[: COLD * BLOCK, :]) + dot(hots, wd[COLD * BLOCK :, :])
        oown[s] = result[:ROWS]
        obuf[s] = result.astype(BF16)
        for dx in (2, 1, 3):
            remote(
                obuf.at[s, pl.ds(dx * ROWS, ROWS), :], dbuf.at[s, dx - 1], d1s.at[s], d1r.at[s],
                dev(at_x(dx), y, z, k),
            ).start()

    for s in range(STEPS):
        remote(dbuf.at[s], dbuf.at[s], d1s.at[s], d1r.at[s], here).wait_recv()
        terms = oown[s]
        for i in range(NX - 1):
            terms = terms + dbuf[s, i].astype(F32)
        ebuf[s, 0] = terms[:, :feat].astype(BF16)
        ebuf[s, 1] = terms[:, feat:].astype(BF16)
        dy = dy_of(s)

        def to_owners():
            for f in range(2):
                remote(
                    ebuf.at[s, f], fbuf.at[dy], d2s.at[s], d2r, dev(x, at_y(dy), z, f)
                ).start()

        if s:
            to_owners()
        else:
            pl.when(k == 1)(to_owners)

            @pl.when(k == 0)
            def _():
                remote(ebuf.at[0, 1], fbuf.at[0], d2z, d2zr, sister).start()
                fbuf[0] = terms[:, :feat].astype(BF16)

    remote(fbuf.at[pl.ds(1, NY - 1)], fbuf.at[pl.ds(1, NY - 1)], a1s, d2r, here).wait_recv()

    @pl.when(k == 1)
    def _():
        remote(fbuf.at[0], fbuf.at[0], d2z, d2zr, here).wait_recv()

    answer = fbuf[0].astype(F32)
    for dy in range(1, NY):
        answer = answer + fbuf[dy].astype(F32)
    out[...] = answer.astype(BF16)

    seven = fbuf.at[pl.ds(1, NY - 1)]
    remote(seven, seven, a1s, d2r, here).wait_send()
    for copy in remote_w:
        copy.wait_send()
    for s in range(STEPS):
        rest = xbuf.at[s, pl.ds(ROWS, TOK - ROWS), :]
        remote(rest, rest, a2s.at[s], a2r.at[s], here).wait_send()
        remote(rbuf.at[s], rbuf.at[s], bs.at[s], br.at[s], here).wait_send()
        most = hbuf.at[s, pl.ds(0, NZ - 1)]
        remote(most, most, cs.at[s], cr.at[s], here).wait_send()
        remote(dbuf.at[s], dbuf.at[s], d1s.at[s], d1r.at[s], here).wait_send()
        if s:
            remote(ebuf.at[s], ebuf.at[s], d2s.at[s], d2r, here).wait_send()

    @pl.when(k == 1)
    def _():
        remote(ebuf.at[0], ebuf.at[0], d2s.at[0], d2r, here).wait_send()
        remote(tokv, tokv, a1z, a1r.at[0], here).wait_send()

    @pl.when(k == 0)
    def _():
        remote(ebuf.at[0, 1], ebuf.at[0, 1], d2z, d2zr, here).wait_send()


def body(*args):
    rows, feat = args[0].shape
    hbm = pl.BlockSpec(memory_space=pl.ANY)
    smem = pl.BlockSpec(memory_space=pltpu.SMEM)
    blocks = args[9].shape[1]
    dma = pltpu.SemaphoreType.DMA
    return pl.pallas_call(
        kernel,
        out_shape=jax.ShapeDtypeStruct((rows, feat), BF16),
        in_specs=[hbm] * 7 + [smem] * 2 + [hbm],
        out_specs=pl.BlockSpec(memory_space=pltpu.VMEM),
        scratch_shapes=[
            pltpu.VMEM((ROWS, feat), BF16),
            pltpu.VMEM((STEPS, TOK, 2 * feat), BF16),
            pltpu.VMEM((2 * feat, COLD * BLOCK), BF16),
            pltpu.VMEM((2 * feat, COLD * BLOCK), BF16),
            pltpu.VMEM((2 * feat, 2 * BLOCK), BF16),
            pltpu.VMEM(((COLD + 1) * BLOCK, 2 * feat), BF16),
            pltpu.VMEM((STEPS * TOK, blocks), jnp.int32),
            pltpu.VMEM((STEPS, TOK, BLOCK), BF16),
            pltpu.VMEM((STEPS, SLOTS, TOK), BF16),
            pltpu.VMEM((STEPS, SLOTS, BLOCK), F32),
            pltpu.VMEM((STEPS, NZ, SLOTS, 2 * BLOCK), BF16),
            pltpu.VMEM((STEPS, NZ, SLOTS, 2 * BLOCK), F32),
            pltpu.VMEM((STEPS, NZ - 1, SLOTS, 2 * BLOCK), BF16),
            pltpu.VMEM((STEPS, NZ, SLOTS, BLOCK), BF16),
            pltpu.VMEM((STEPS, TOK, 2 * feat), BF16),
            pltpu.VMEM((STEPS, ROWS, 2 * feat), F32),
            pltpu.VMEM((STEPS, NX - 1, ROWS, 2 * feat), BF16),
            pltpu.VMEM((STEPS, 2, ROWS, feat), BF16),
            pltpu.VMEM((NY, ROWS, feat), BF16),
            dma, dma, dma((6,)), dma((6,)), dma((6,)),
            dma, dma, dma((STEPS,)), dma((STEPS,)), dma((STEPS,)),
            dma((STEPS,)), dma((STEPS,)), dma((STEPS,)), dma((STEPS,)),
            dma((STEPS,)), dma((STEPS,)), dma((STEPS,)), dma, dma, dma,
        ],
        compiler_params=pltpu.CompilerParams(collective_id=0, has_side_effects=True),
    )(*args)


def solution(mesh):
    return jax.shard_map(
        body,
        mesh=mesh,
        in_specs=(
            P("cold", "hot"),
            P("hot", "cold"),
            P("hot", "cold"),
            P("cold", "hot"),
            P("hot", "cold"),
            P("hot", "cold"),
            P("cold", "hot"),
            P(),
            P(),
            P(),
        ),
        out_specs=P("cold", "hot"),
        check_vma=False,
    )
```

```python
import jax
import jax.numpy as jnp
from jax import lax
from jax.experimental import pallas as pl
from jax.experimental.pallas import tpu as pltpu
from jax.sharding import PartitionSpec as P

BLOCK = 128
NX, NY, NZ = 4, 8, 8
STEPS = 4
CAP = 8
ROWS = 16
TOK = NX * ROWS
SLOTS = NX * CAP
COLD = 6
F32, BF16 = jnp.float32, jnp.bfloat16
ORDER = ((0, 7, 5, 2), (1, 6, 4, 3))
CORE_OF = tuple(0 if dy in ORDER[0] else 1 for dy in range(NY))
SEND_ORDER = (0, 1, 7, 6, 2, 3, 5, 4)
OWN = ORDER[0].index(0)
FAR_FIRST = (4, 3, 5, 2, 6, 1, 7)
MESH = pl.DeviceIdType.MESH


def dot(a, b):
    return jnp.dot(a, b, preferred_element_type=F32)


def dot_t(a, b):
    return lax.dot_general(a, b, (((0,), (0,)), ((), ())), preferred_element_type=F32)


def kernel(
    tok, hot_gate, hot_up, hot_down, cold_gate, cold_up, cold_down, hot_ids, cold_ids, mask,
    out,
    tokv, xbuf, wcg, wcu, wh, wd, maskv, hot_s, cold_s, hits, units, ptab, pmat, mz, sbuf, sown, rbuf, hbuf, obuf, oown, dbuf, ebuf, fbuf,
    xy_in, z_in, tok_sem, mask_sem, ids_sem, wl_sem, ws_sem, wr_sem,
    a1s, a1z, a1r, a2s, a2r, bs, br, cs, cr, d1s, d1r, d2s, d2z, d2r, d2zr,
):
    hot, cold = lax.axis_index("hot"), lax.axis_index("cold")
    z, k = lax.div(hot, 2), lax.rem(hot, 2)
    x, y = lax.div(cold, NY), lax.rem(cold, NY)
    feat = tok.shape[1]

    def dev(px, py, pz, pk):
        return {"hot": pz * 2 + pk, "cold": px * NY + py}

    def at_x(d):
        return lax.rem(x + (d % NX), NX)

    def at_y(d):
        return lax.rem(y + NY + d, NY)

    def at_z(d):
        return lax.rem(z + (d % NZ), NZ)

    def dy_of(s):
        return ORDER[0][s] + k * (ORDER[1][s] - ORDER[0][s])

    def remote(src, dst, send, recv, to):
        return pltpu.make_async_remote_copy(
            src_ref=src, dst_ref=dst, send_sem=send, recv_sem=recv, device_id=to, device_id_type=MESH
        )

    here = dev(x, y, z, k)
    sister = dev(x, y, z, 1 - k)
    cols = pl.ds(pl.multiple_of(k * feat, feat), feat)
    mine = pl.ds(pl.multiple_of(k * feat, feat), feat)

    tok_load = pltpu.make_async_copy(tok, tokv, tok_sem)
    tok_load.start()

    barrier = pltpu.get_barrier_semaphore()

    def greet(to):
        pl.semaphore_signal(barrier, inc=1, device_id=to, device_id_type=MESH)

    greet(sister)
    for d in range(1, NY):
        greet(dev(x, at_y(d), z, 1))
    for d in range(1, NX):
        greet(dev(at_x(d), y, z, 1))
    for d in FAR_FIRST:
        greet(dev(x, y, at_z(d), 0))

    mask_load = pltpu.make_async_copy(mask, maskv, mask_sem)
    hot_load = pltpu.make_async_copy(hot_ids, hot_s, ids_sem.at[0])
    cold_load = pltpu.make_async_copy(cold_ids, cold_s, ids_sem.at[1])
    pieces = (
        (cold_gate, wcg.at[mine, :]),
        (cold_up, wcu.at[mine, :]),
        (hot_gate, wh.at[mine, pl.ds(0, BLOCK)]),
        (hot_up, wh.at[mine, pl.ds(BLOCK, BLOCK)]),
        (cold_down, wd.at[pl.ds(0, COLD * BLOCK), cols]),
        (hot_down, wd.at[pl.ds(COLD * BLOCK, BLOCK), cols]),
    )
    local_w = [pltpu.make_async_copy(a, b, wl_sem.at[i]) for i, (a, b) in enumerate(pieces)]
    remote_w = [remote(a, b, ws_sem.at[i], wr_sem.at[i], sister) for i, (a, b) in enumerate(pieces)]
    tok_load.wait()

    @pl.when(k == 1)
    def _():
        pl.semaphore_wait(barrier, 2 * (NY - 1) + 2 * (NX - 1) + 1)
        pl.semaphore_signal(xy_in, inc=1, device_id=sister, device_id_type=MESH)

    @pl.when(k == 0)
    def _():
        pl.semaphore_wait(xy_in, 1)

    for dy in SEND_ORDER:
        core = CORE_OF[dy]
        s = ORDER[core].index(dy)
        spot = xbuf.at[s, pl.ds(0, ROWS), cols]
        if dy:
            remote(tokv, spot, a1s, a1r.at[s], dev(x, at_y(-dy), z, core)).start()
        else:

            @pl.when(k == 0)
            def _():
                pltpu.make_async_copy(tok, xbuf.at[OWN, pl.ds(0, ROWS), pl.ds(0, feat)], a1r.at[OWN]).start()

            @pl.when(k == 1)
            def _():
                remote(
                    tokv, xbuf.at[OWN, pl.ds(0, ROWS), pl.ds(feat, feat)], a1z, a1r.at[OWN], sister
                ).start()

    for copy in (mask_load, hot_load, cold_load):
        copy.start()
    for copy in local_w[:4] + remote_w[:4] + local_w[4:]:
        copy.start()

    def spread(s):
        head = xbuf.at[s, pl.ds(0, ROWS), :]
        remote(head, head, a2s.at[s], a1r.at[s], here).wait_recv()
        for dx in (2, 1, 3):
            remote(
                head, xbuf.at[s, pl.ds(dx * ROWS, ROWS), :], a2s.at[s], a2r.at[s], dev(at_x(-dx), y, z, k)
            ).start()

    def gate_up(s):
        rest = xbuf.at[s, pl.ds(ROWS, TOK - ROWS), :]
        remote(rest, rest, a2s.at[s], a2r.at[s], here).wait_recv()
        if s == 0:
            for i in range(4):
                local_w[i].wait()
                remote_w[i].wait_recv()
        rows = xbuf[s]
        picked = dot(pmat[s], rows).astype(BF16)
        gates, ups = dot(picked, wcg[...]), dot(picked, wcu[...])
        hots = dot(rows, wh[...])
        for j in range(NZ):
            if j < COLD:
                part = slice(j * BLOCK, (j + 1) * BLOCK)
                gate, up = gates[:, part], ups[:, part]
            else:
                part = slice((j - COLD) * SLOTS, (j - COLD + 1) * SLOTS)
                gate, up = hots[part, :BLOCK], hots[part, BLOCK:]
            sown[s, j, :, :BLOCK] = gate
            sown[s, j, :, BLOCK:] = up
            sbuf[s, j, :, :BLOCK] = gate.astype(BF16)
            sbuf[s, j, :, BLOCK:] = up.astype(BF16)
        if s == 0:

            @pl.when(k == 0)
            def _():
                pl.semaphore_wait(barrier, 2 * (NZ - 1) + 1)
                pl.semaphore_signal(z_in, inc=1, device_id=sister, device_id_type=MESH)

            @pl.when(k == 1)
            def _():
                pl.semaphore_wait(z_in, 1)

        for dz in FAR_FIRST:
            remote(
                sbuf.at[s, at_z(dz)], rbuf.at[s, dz - 1], bs.at[s], br.at[s], dev(x, y, at_z(dz), k)
            ).start()

    def share(s):
        remote(rbuf.at[s], rbuf.at[s], bs.at[s], br.at[s], here).wait_recv()
        terms = sown[s, z]
        for i in range(NZ - 1):
            terms = terms + rbuf[s, i].astype(F32)
        gate, up = terms[:, :BLOCK], terms[:, BLOCK:]
        hidden = gate / (1.0 + jnp.exp(-gate)) * up * mz[s]
        hbuf[s, z] = hidden.astype(BF16)
        for dz in FAR_FIRST:
            remote(
                hbuf.at[s, z], hbuf.at[s, z], cs.at[s], cr.at[s], dev(x, y, at_z(dz), k)
            ).start()

    spread(0)

    for copy in (mask_load, hot_load, cold_load):
        copy.wait()
    bits = maskv[...].astype(F32).astype(BF16)
    blocks = maskv.shape[0]
    block_no = lax.broadcasted_iota(jnp.int32, (blocks, BLOCK), 0)
    cold_sel = jnp.zeros((blocks, BLOCK), F32)
    for j in range(COLD):
        cold_sel = cold_sel + jnp.where(block_no == cold_s[cold * COLD + j], 1.0, 0.0)
    unit_id = jnp.where(z < COLD, cold_s[cold * COLD + jnp.minimum(z, COLD - 1)], hot_s[cold])
    unit_sel = jnp.where(block_no == unit_id, 1.0, 0.0)
    hits[...] = jnp.minimum(dot_t(bits, cold_sel.astype(BF16)), 1.0)
    units[...] = dot_t(bits, unit_sel.astype(BF16))

    def in_order(ref):
        starts = [(at_x(dx) * NY + at_y(dy_of(s))) * ROWS for s in range(STEPS) for dx in range(NX)]
        return jnp.concatenate([ref[pl.ds(pl.multiple_of(i, ROWS), ROWS), :] for i in starts], axis=0)

    hit, unit_bit = in_order(hits), in_order(units)
    total = STEPS * TOK
    row = lax.broadcasted_iota(jnp.int32, (total, total), 0)
    col = lax.broadcasted_iota(jnp.int32, (total, total), 1)
    earlier = (lax.div(row, ROWS) == lax.div(col, ROWS)) & (col < row)
    slot = dot(jnp.where(earlier, 1.0, 0.0).astype(BF16), hit.astype(BF16))
    row = lax.broadcasted_iota(jnp.int32, (total, BLOCK), 0)
    lane = lax.broadcasted_iota(jnp.int32, (total, BLOCK), 1)
    base = lax.rem(lax.div(row, ROWS), NX) * CAP
    chosen = jnp.where((slot + base.astype(F32) == lane.astype(F32)) & (hit > 0.5), 1.0, 0.0)
    for s in range(STEPS):
        step_rows = slice(s * TOK, (s + 1) * TOK)
        pick = chosen[step_rows]
        ptab[s] = pick.astype(BF16)
        turned = jnp.transpose(pick)[:SLOTS].astype(BF16)
        pmat[s] = turned
        tokens_bit = unit_bit[step_rows]
        slot_bit = dot(turned, tokens_bit.astype(BF16))
        half_bit = jnp.where(z == COLD, tokens_bit[:SLOTS], tokens_bit[SLOTS:])
        mz[s] = jnp.where(z < COLD, slot_bit, half_bit)

    spread(1)
    gate_up(0)
    spread(3)
    spread(2)
    for copy in remote_w[4:]:
        copy.start()
    def down(s):
        most = hbuf.at[s, pl.ds(0, NZ - 1)]
        remote(most, most, cs.at[s], cr.at[s], here).wait_recv()
        if s == 0:
            for i in (4, 5):
                local_w[i].wait()
                remote_w[i].wait_recv()
        colds = jnp.concatenate([hbuf[s, j] for j in range(COLD)], axis=1)
        placed = dot(ptab[s][:, :SLOTS], colds).astype(BF16)
        hots = jnp.concatenate([hbuf[s, COLD], hbuf[s, COLD + 1]], axis=0)
        result = dot(placed, wd[: COLD * BLOCK, :]) + dot(hots, wd[COLD * BLOCK :, :])
        oown[s] = result[:ROWS]
        obuf[s] = result.astype(BF16)
        for dx in (2, 1, 3):
            remote(
                obuf.at[s, pl.ds(dx * ROWS, ROWS), :], dbuf.at[s, dx - 1], d1s.at[s], d1r.at[s],
                dev(at_x(dx), y, z, k),
            ).start()

    def collect(s):
        remote(dbuf.at[s], dbuf.at[s], d1s.at[s], d1r.at[s], here).wait_recv()
        terms = oown[s]
        for i in range(NX - 1):
            terms = terms + dbuf[s, i].astype(F32)
        ebuf[s, 0] = terms[:, :feat].astype(BF16)
        ebuf[s, 1] = terms[:, feat:].astype(BF16)
        dy = dy_of(s)

        def to_owners():
            for f in range(2):
                remote(
                    ebuf.at[s, f], fbuf.at[dy], d2s.at[s], d2r, dev(x, at_y(dy), z, f)
                ).start()

        if s != OWN:
            to_owners()
        else:
            pl.when(k == 1)(to_owners)

            @pl.when(k == 0)
            def _():
                remote(ebuf.at[OWN, 1], fbuf.at[0], d2z, d2zr, sister).start()
                fbuf[0] = terms[:, :feat].astype(BF16)

    gate_up(1)
    share(0)
    gate_up(2)
    share(1)
    gate_up(3)
    share(2)
    down(0)
    share(3)
    down(1)
    collect(0)
    down(2)
    down(3)
    collect(1)
    collect(2)
    collect(3)

    remote(fbuf.at[pl.ds(1, NY - 1)], fbuf.at[pl.ds(1, NY - 1)], a1s, d2r, here).wait_recv()

    @pl.when(k == 1)
    def _():
        remote(fbuf.at[0], fbuf.at[0], d2z, d2zr, here).wait_recv()

    answer = fbuf[0].astype(F32)
    for dy in range(1, NY):
        answer = answer + fbuf[dy].astype(F32)
    out[...] = answer.astype(BF16)

    seven = fbuf.at[pl.ds(1, NY - 1)]
    remote(seven, seven, a1s, d2r, here).wait_send()
    for copy in remote_w:
        copy.wait_send()
    for s in range(STEPS):
        rest = xbuf.at[s, pl.ds(ROWS, TOK - ROWS), :]
        remote(rest, rest, a2s.at[s], a2r.at[s], here).wait_send()
        remote(rbuf.at[s], rbuf.at[s], bs.at[s], br.at[s], here).wait_send()
        most = hbuf.at[s, pl.ds(0, NZ - 1)]
        remote(most, most, cs.at[s], cr.at[s], here).wait_send()
        remote(dbuf.at[s], dbuf.at[s], d1s.at[s], d1r.at[s], here).wait_send()
        if s != OWN:
            remote(ebuf.at[s], ebuf.at[s], d2s.at[s], d2r, here).wait_send()

    @pl.when(k == 1)
    def _():
        remote(ebuf.at[OWN], ebuf.at[OWN], d2s.at[OWN], d2r, here).wait_send()
        remote(tokv, tokv, a1z, a1r.at[OWN], here).wait_send()

    @pl.when(k == 0)
    def _():
        remote(ebuf.at[OWN, 1], ebuf.at[OWN, 1], d2z, d2zr, here).wait_send()


def body(*args):
    rows, feat = args[0].shape
    hbm = pl.BlockSpec(memory_space=pl.ANY)
    args = (*args[:9], args[9].T)
    blocks, tokens = args[9].shape
    dma = pltpu.SemaphoreType.DMA
    args = tuple(pltpu.with_memory_space_constraint(a, pltpu.HBM) for a in args)
    return pl.pallas_call(
        kernel,
        out_shape=jax.ShapeDtypeStruct((rows, feat), BF16),
        in_specs=[hbm] * 10,
        out_specs=pl.BlockSpec(memory_space=pltpu.VMEM),
        scratch_shapes=[
            pltpu.VMEM((ROWS, feat), BF16),
            pltpu.VMEM((STEPS, TOK, 2 * feat), BF16),
            pltpu.VMEM((2 * feat, COLD * BLOCK), BF16),
            pltpu.VMEM((2 * feat, COLD * BLOCK), BF16),
            pltpu.VMEM((2 * feat, 2 * BLOCK), BF16),
            pltpu.VMEM(((COLD + 1) * BLOCK, 2 * feat), BF16),
            pltpu.VMEM((blocks, tokens), jnp.int32),
            pltpu.SMEM(args[7].shape, jnp.int32),
            pltpu.SMEM(args[8].shape, jnp.int32),
            pltpu.VMEM((tokens, BLOCK), F32),
            pltpu.VMEM((tokens, BLOCK), F32),
            pltpu.VMEM((STEPS, TOK, BLOCK), BF16),
            pltpu.VMEM((STEPS, SLOTS, TOK), BF16),
            pltpu.VMEM((STEPS, SLOTS, BLOCK), F32),
            pltpu.VMEM((STEPS, NZ, SLOTS, 2 * BLOCK), BF16),
            pltpu.VMEM((STEPS, NZ, SLOTS, 2 * BLOCK), F32),
            pltpu.VMEM((STEPS, NZ - 1, SLOTS, 2 * BLOCK), BF16),
            pltpu.VMEM((STEPS, NZ, SLOTS, BLOCK), BF16),
            pltpu.VMEM((STEPS, TOK, 2 * feat), BF16),
            pltpu.VMEM((STEPS, ROWS, 2 * feat), F32),
            pltpu.VMEM((STEPS, NX - 1, ROWS, 2 * feat), BF16),
            pltpu.VMEM((STEPS, 2, ROWS, feat), BF16),
            pltpu.VMEM((NY, ROWS, feat), BF16),
            pltpu.SemaphoreType.REGULAR, pltpu.SemaphoreType.REGULAR,
            dma, dma, dma((2,)), dma((6,)), dma((6,)), dma((6,)),
            dma, dma, dma((STEPS,)), dma((STEPS,)), dma((STEPS,)),
            dma((STEPS,)), dma((STEPS,)), dma((STEPS,)), dma((STEPS,)),
            dma((STEPS,)), dma((STEPS,)), dma((STEPS,)), dma, dma, dma,
        ],
        compiler_params=pltpu.CompilerParams(collective_id=0, has_side_effects=True, vmem_limit_bytes=32 * 2**20),
    )(*args)


def solution(mesh):
    return jax.shard_map(
        body,
        mesh=mesh,
        in_specs=(
            P("cold", "hot"),
            P("hot", "cold"),
            P("hot", "cold"),
            P("cold", "hot"),
            P("hot", "cold"),
            P("hot", "cold"),
            P("cold", "hot"),
            P(),
            P(),
            P(),
        ),
        out_specs=P("cold", "hot"),
        check_vma=False,
    )
```

```python
import jax
import jax.numpy as jnp
from jax import lax
from jax.experimental import pallas as pl
from jax.experimental.pallas import tpu as pltpu
from jax.sharding import PartitionSpec as P

BLOCK = 128
NX, NY, NZ = 4, 8, 8
STEPS = 4
CAP = 8
ROWS = 16
TOK = NX * ROWS
SLOTS = NX * CAP
COLD = 6
F32, BF16 = jnp.float32, jnp.bfloat16
ORDER = ((0, 7, 5, 2), (1, 6, 4, 3))
CORE_OF = tuple(0 if dy in ORDER[0] else 1 for dy in range(NY))
SEND_ORDER = (0, 1, 7, 6, 2, 3, 5, 4)
OWN = ORDER[0].index(0)
LAST = STEPS - 1
FAR_FIRST = (4, 3, 5, 2, 6, 1, 7)
MESH = pl.DeviceIdType.MESH


def dot(a, b):
    return jnp.dot(a, b, preferred_element_type=F32)


def dot_t(a, b):
    return lax.dot_general(a, b, (((0,), (0,)), ((), ())), preferred_element_type=F32)


def kernel(
    tok, hot_gate, hot_up, hot_down, cold_gate, cold_up, cold_down, hot_ids, cold_ids, mask,
    out,
    tokv, xbuf, wcg, wcu, wh, wd, maskv, hot_s, cold_s, hits, units, ptab, pmat, mz, sbuf, sown, rbuf, hbuf, obuf, oown, dbuf, ebuf, fbuf,
    xy_in, z_in, tok_sem, mask_sem, ids_sem, wl_sem, ws_sem, wr_sem,
    a1s, a1z, a1r, a2s, a2r, bs, br, cs, cr, d1s, d1r, d2s, d2z, d2r, d2zr,
):
    hot, cold = lax.axis_index("hot"), lax.axis_index("cold")
    z, k = lax.div(hot, 2), lax.rem(hot, 2)
    x, y = lax.div(cold, NY), lax.rem(cold, NY)
    feat = tok.shape[1]

    def dev(px, py, pz, pk):
        return {"hot": pz * 2 + pk, "cold": px * NY + py}

    def at_x(d):
        return lax.rem(x + (d % NX), NX)

    def at_y(d):
        return lax.rem(y + NY + d, NY)

    def at_z(d):
        return lax.rem(z + (d % NZ), NZ)

    def dy_of(s):
        return ORDER[0][s] + k * (ORDER[1][s] - ORDER[0][s])

    def remote(src, dst, send, recv, to):
        return pltpu.make_async_remote_copy(
            src_ref=src, dst_ref=dst, send_sem=send, recv_sem=recv, device_id=to, device_id_type=MESH
        )

    def parts_of(s):
        if s == LAST:
            return ((STEPS, slice(feat, 2 * feat)), (s, slice(0, feat)))
        return ((s, slice(0, 2 * feat)),)

    here = dev(x, y, z, k)
    sister = dev(x, y, z, 1 - k)
    cols = pl.ds(pl.multiple_of(k * feat, feat), feat)
    mine = pl.ds(pl.multiple_of(k * feat, feat), feat)

    tok_load = pltpu.make_async_copy(tok, tokv, tok_sem)
    tok_load.start()

    barrier = pltpu.get_barrier_semaphore()

    def greet(to):
        pl.semaphore_signal(barrier, inc=1, device_id=to, device_id_type=MESH)

    greet(sister)
    for d in range(1, NY):
        greet(dev(x, at_y(d), z, 1))
    for d in range(1, NX):
        greet(dev(at_x(d), y, z, 1))
    for d in FAR_FIRST:
        greet(dev(x, y, at_z(d), 0))

    mask_load = pltpu.make_async_copy(mask, maskv, mask_sem)
    hot_load = pltpu.make_async_copy(hot_ids, hot_s, ids_sem.at[0])
    cold_load = pltpu.make_async_copy(cold_ids, cold_s, ids_sem.at[1])
    pieces = (
        (cold_gate, wcg.at[mine, :]),
        (cold_up, wcu.at[mine, :]),
        (hot_gate, wh.at[mine, pl.ds(0, BLOCK)]),
        (hot_up, wh.at[mine, pl.ds(BLOCK, BLOCK)]),
        (cold_down, wd.at[pl.ds(0, COLD * BLOCK), cols]),
        (hot_down, wd.at[pl.ds(COLD * BLOCK, BLOCK), cols]),
    )
    local_w = [pltpu.make_async_copy(a, b, wl_sem.at[i]) for i, (a, b) in enumerate(pieces)]
    remote_w = [remote(a, b, ws_sem.at[i], wr_sem.at[i], sister) for i, (a, b) in enumerate(pieces)]
    tok_load.wait()

    @pl.when(k == 1)
    def _():
        pl.semaphore_wait(barrier, 2 * (NY - 1) + 2 * (NX - 1) + 1)
        pl.semaphore_signal(xy_in, inc=1, device_id=sister, device_id_type=MESH)

    @pl.when(k == 0)
    def _():
        pl.semaphore_wait(xy_in, 1)

    for dy in SEND_ORDER:
        core = CORE_OF[dy]
        s = ORDER[core].index(dy)
        spot = xbuf.at[s, pl.ds(0, ROWS), cols]
        if dy:
            remote(tokv, spot, a1s, a1r.at[s], dev(x, at_y(-dy), z, core)).start()
        else:

            @pl.when(k == 0)
            def _():
                pltpu.make_async_copy(tok, xbuf.at[OWN, pl.ds(0, ROWS), pl.ds(0, feat)], a1r.at[OWN]).start()

            @pl.when(k == 1)
            def _():
                remote(
                    tokv, xbuf.at[OWN, pl.ds(0, ROWS), pl.ds(feat, feat)], a1z, a1r.at[OWN], sister
                ).start()

    for copy in (mask_load, hot_load, cold_load):
        copy.start()
    for copy in local_w[:4] + remote_w[:4] + local_w[4:]:
        copy.start()

    def spread(s):
        head = xbuf.at[s, pl.ds(0, ROWS), :]
        remote(head, head, a2s.at[s], a1r.at[s], here).wait_recv()
        for dx in (2, 1, 3):
            remote(
                head, xbuf.at[s, pl.ds(dx * ROWS, ROWS), :], a2s.at[s], a2r.at[s], dev(at_x(-dx), y, z, k)
            ).start()

    def gate_up(s):
        rest = xbuf.at[s, pl.ds(ROWS, TOK - ROWS), :]
        remote(rest, rest, a2s.at[s], a2r.at[s], here).wait_recv()
        if s == 0:
            for i in range(4):
                local_w[i].wait()
                remote_w[i].wait_recv()
        rows = xbuf[s]
        picked = dot(pmat[s], rows).astype(BF16)
        gates, ups = dot(picked, wcg[...]), dot(picked, wcu[...])
        hots = dot(rows, wh[...])
        for j in range(NZ):
            if j < COLD:
                part = slice(j * BLOCK, (j + 1) * BLOCK)
                gate, up = gates[:, part], ups[:, part]
            else:
                part = slice((j - COLD) * SLOTS, (j - COLD + 1) * SLOTS)
                gate, up = hots[part, :BLOCK], hots[part, BLOCK:]
            sown[s, j, :, :BLOCK] = gate
            sown[s, j, :, BLOCK:] = up
            sbuf[s, j, :, :BLOCK] = gate.astype(BF16)
            sbuf[s, j, :, BLOCK:] = up.astype(BF16)
        if s == 0:

            @pl.when(k == 0)
            def _():
                pl.semaphore_wait(barrier, 2 * (NZ - 1) + 1)
                pl.semaphore_signal(z_in, inc=1, device_id=sister, device_id_type=MESH)

            @pl.when(k == 1)
            def _():
                pl.semaphore_wait(z_in, 1)

        for dz in FAR_FIRST:
            remote(
                sbuf.at[s, at_z(dz)], rbuf.at[s, dz - 1], bs.at[s], br.at[s], dev(x, y, at_z(dz), k)
            ).start()

    def share(s):
        remote(rbuf.at[s], rbuf.at[s], bs.at[s], br.at[s], here).wait_recv()
        terms = sown[s, z]
        for i in range(NZ - 1):
            terms = terms + rbuf[s, i].astype(F32)
        gate, up = terms[:, :BLOCK], terms[:, BLOCK:]
        hidden = gate / (1.0 + jnp.exp(-gate)) * up * mz[s]
        hbuf[s, z] = hidden.astype(BF16)
        for i in range(NZ - 1):
            to = i + jnp.where(z <= i, 1, 0)
            remote(hbuf.at[s, z], hbuf.at[s, z], cs.at[s], cr.at[s], dev(x, y, to, k)).start()

    spread(0)

    for copy in (mask_load, hot_load, cold_load):
        copy.wait()
    bits = maskv[...].astype(F32).astype(BF16)
    blocks = maskv.shape[0]
    block_no = lax.broadcasted_iota(jnp.int32, (blocks, BLOCK), 0)
    cold_sel = jnp.zeros((blocks, BLOCK), F32)
    for j in range(COLD):
        cold_sel = cold_sel + jnp.where(block_no == cold_s[cold * COLD + j], 1.0, 0.0)
    unit_id = jnp.where(z < COLD, cold_s[cold * COLD + jnp.minimum(z, COLD - 1)], hot_s[cold])
    unit_sel = jnp.where(block_no == unit_id, 1.0, 0.0)
    hits[...] = jnp.minimum(dot_t(bits, cold_sel.astype(BF16)), 1.0)
    units[...] = dot_t(bits, unit_sel.astype(BF16))

    def in_order(ref):
        starts = [(at_x(dx) * NY + at_y(dy_of(s))) * ROWS for s in range(STEPS) for dx in range(NX)]
        return jnp.concatenate([ref[pl.ds(pl.multiple_of(i, ROWS), ROWS), :] for i in starts], axis=0)

    hit, unit_bit = in_order(hits), in_order(units)
    total = STEPS * TOK
    row = lax.broadcasted_iota(jnp.int32, (total, total), 0)
    col = lax.broadcasted_iota(jnp.int32, (total, total), 1)
    earlier = (lax.div(row, ROWS) == lax.div(col, ROWS)) & (col < row)
    slot = dot(jnp.where(earlier, 1.0, 0.0).astype(BF16), hit.astype(BF16))
    row = lax.broadcasted_iota(jnp.int32, (total, BLOCK), 0)
    lane = lax.broadcasted_iota(jnp.int32, (total, BLOCK), 1)
    base = lax.rem(lax.div(row, ROWS), NX) * CAP
    chosen = jnp.where((slot + base.astype(F32) == lane.astype(F32)) & (hit > 0.5), 1.0, 0.0)
    for s in range(STEPS):
        step_rows = slice(s * TOK, (s + 1) * TOK)
        pick = chosen[step_rows]
        ptab[s] = pick.astype(BF16)
        turned = jnp.transpose(pick)[:SLOTS].astype(BF16)
        pmat[s] = turned
        tokens_bit = unit_bit[step_rows]
        slot_bit = dot(turned, tokens_bit.astype(BF16))
        half_bit = jnp.where(z == COLD, tokens_bit[:SLOTS], tokens_bit[SLOTS:])
        mz[s] = jnp.where(z < COLD, slot_bit, half_bit)

    spread(1)
    gate_up(0)
    spread(3)
    spread(2)
    for copy in remote_w[4:]:
        copy.start()
    def down(s):
        most = hbuf.at[s, pl.ds(0, NZ - 1)]
        remote(most, most, cs.at[s], cr.at[s], here).wait_recv()
        if s == 0:
            for i in (4, 5):
                local_w[i].wait()
                remote_w[i].wait_recv()
        colds = jnp.concatenate([hbuf[s, j] for j in range(COLD)], axis=1)
        placed = dot(ptab[s][:, :SLOTS], colds).astype(BF16)
        hots = jnp.concatenate([hbuf[s, COLD], hbuf[s, COLD + 1]], axis=0)
        for index, part in parts_of(s):
            result = dot(placed, wd[: COLD * BLOCK, part]) + dot(hots, wd[COLD * BLOCK :, part])
            oown[s, :, part] = result[:ROWS]
            obuf[s, :, part] = result.astype(BF16)
            for dx in (2, 1, 3):
                remote(
                    obuf.at[s, pl.ds(dx * ROWS, ROWS), part], dbuf.at[s, dx - 1, :, part], d1s.at[index],
                    d1r.at[index], dev(at_x(dx), y, z, k),
                ).start()

    def collect(s):
        dy = dy_of(s)
        for index, part in parts_of(s):
            sums = dbuf.at[s, :, :, part]
            remote(sums, sums, d1s.at[index], d1r.at[index], here).wait_recv()
            terms = oown[s, :, part]
            for i in range(NX - 1):
                terms = terms + dbuf[s, i, :, part].astype(F32)
            for f in range(2):
                if index == s and s == LAST and f == 1:
                    continue
                if index != s and f == 0:
                    continue
                piece = terms[:, f * feat : (f + 1) * feat] if terms.shape[1] > feat else terms
                ebuf[s, f] = piece.astype(BF16)
                if s == LAST:
                    remote(ebuf.at[s, f], fbuf.at[dy], d2s.at[s], d2r, dev(x, at_y(dy), z, f)).start()
        if s == LAST:
            return

        def to_owners():
            for f in range(2):
                remote(
                    ebuf.at[s, f], fbuf.at[dy], d2s.at[s], d2r, dev(x, at_y(dy), z, f)
                ).start()

        if s != OWN:
            to_owners()
        else:
            pl.when(k == 1)(to_owners)

            @pl.when(k == 0)
            def _():
                remote(ebuf.at[OWN, 1], fbuf.at[0], d2z, d2zr, sister).start()
                fbuf[0] = ebuf[OWN, 0]

    gate_up(1)
    share(0)
    gate_up(2)
    share(1)
    gate_up(3)
    share(2)
    down(0)
    share(3)
    down(1)
    collect(0)
    down(2)
    down(3)
    collect(1)
    collect(2)
    collect(3)

    remote(fbuf.at[pl.ds(1, NY - 1)], fbuf.at[pl.ds(1, NY - 1)], a1s, d2r, here).wait_recv()

    @pl.when(k == 1)
    def _():
        remote(fbuf.at[0], fbuf.at[0], d2z, d2zr, here).wait_recv()

    answer = fbuf[0].astype(F32)
    for dy in range(1, NY):
        answer = answer + fbuf[dy].astype(F32)
    out[...] = answer.astype(BF16)

    seven = fbuf.at[pl.ds(1, NY - 1)]
    remote(seven, seven, a1s, d2r, here).wait_send()
    for copy in remote_w:
        copy.wait_send()
    for s in range(STEPS):
        rest = xbuf.at[s, pl.ds(ROWS, TOK - ROWS), :]
        remote(rest, rest, a2s.at[s], a2r.at[s], here).wait_send()
        remote(rbuf.at[s], rbuf.at[s], bs.at[s], br.at[s], here).wait_send()
        most = hbuf.at[s, pl.ds(0, NZ - 1)]
        remote(most, most, cs.at[s], cr.at[s], here).wait_send()
        for index, part in parts_of(s):
            sums = dbuf.at[s, :, :, part]
            remote(sums, sums, d1s.at[index], d1r.at[index], here).wait_send()
        if s != OWN:
            remote(ebuf.at[s], ebuf.at[s], d2s.at[s], d2r, here).wait_send()

    @pl.when(k == 1)
    def _():
        remote(ebuf.at[OWN], ebuf.at[OWN], d2s.at[OWN], d2r, here).wait_send()
        remote(tokv, tokv, a1z, a1r.at[OWN], here).wait_send()

    @pl.when(k == 0)
    def _():
        remote(ebuf.at[OWN, 1], ebuf.at[OWN, 1], d2z, d2zr, here).wait_send()


def body(*args):
    rows, feat = args[0].shape
    hbm = pl.BlockSpec(memory_space=pl.ANY)
    args = (*args[:9], args[9].T)
    blocks, tokens = args[9].shape
    dma = pltpu.SemaphoreType.DMA
    args = tuple(pltpu.with_memory_space_constraint(a, pltpu.HBM) for a in args)
    return pl.pallas_call(
        kernel,
        out_shape=jax.ShapeDtypeStruct((rows, feat), BF16),
        in_specs=[hbm] * 10,
        out_specs=pl.BlockSpec(memory_space=pltpu.VMEM),
        scratch_shapes=[
            pltpu.VMEM((ROWS, feat), BF16),
            pltpu.VMEM((STEPS, TOK, 2 * feat), BF16),
            pltpu.VMEM((2 * feat, COLD * BLOCK), BF16),
            pltpu.VMEM((2 * feat, COLD * BLOCK), BF16),
            pltpu.VMEM((2 * feat, 2 * BLOCK), BF16),
            pltpu.VMEM(((COLD + 1) * BLOCK, 2 * feat), BF16),
            pltpu.VMEM((blocks, tokens), jnp.int32),
            pltpu.SMEM(args[7].shape, jnp.int32),
            pltpu.SMEM(args[8].shape, jnp.int32),
            pltpu.VMEM((tokens, BLOCK), F32),
            pltpu.VMEM((tokens, BLOCK), F32),
            pltpu.VMEM((STEPS, TOK, BLOCK), BF16),
            pltpu.VMEM((STEPS, SLOTS, TOK), BF16),
            pltpu.VMEM((STEPS, SLOTS, BLOCK), F32),
            pltpu.VMEM((STEPS, NZ, SLOTS, 2 * BLOCK), BF16),
            pltpu.VMEM((STEPS, NZ, SLOTS, 2 * BLOCK), F32),
            pltpu.VMEM((STEPS, NZ - 1, SLOTS, 2 * BLOCK), BF16),
            pltpu.VMEM((STEPS, NZ, SLOTS, BLOCK), BF16),
            pltpu.VMEM((STEPS, TOK, 2 * feat), BF16),
            pltpu.VMEM((STEPS, ROWS, 2 * feat), F32),
            pltpu.VMEM((STEPS, NX - 1, ROWS, 2 * feat), BF16),
            pltpu.VMEM((STEPS, 2, ROWS, feat), BF16),
            pltpu.VMEM((NY, ROWS, feat), BF16),
            pltpu.SemaphoreType.REGULAR, pltpu.SemaphoreType.REGULAR,
            dma, dma, dma((2,)), dma((6,)), dma((6,)), dma((6,)),
            dma, dma, dma((STEPS,)), dma((STEPS,)), dma((STEPS,)),
            dma((STEPS,)), dma((STEPS,)), dma((STEPS,)), dma((STEPS,)),
            dma((STEPS + 1,)), dma((STEPS + 1,)), dma((STEPS,)), dma, dma, dma,
        ],
        compiler_params=pltpu.CompilerParams(collective_id=0, has_side_effects=True, vmem_limit_bytes=32 * 2**20),
    )(*args)


def solution(mesh):
    return jax.shard_map(
        body,
        mesh=mesh,
        in_specs=(
            P("cold", "hot"),
            P("hot", "cold"),
            P("hot", "cold"),
            P("cold", "hot"),
            P("hot", "cold"),
            P("hot", "cold"),
            P("cold", "hot"),
            P(),
            P(),
            P(),
        ),
        out_specs=P("cold", "hot"),
        check_vma=False,
    )
```

```python
import jax
import jax.numpy as jnp
from jax import lax
from jax.experimental import pallas as pl
from jax.experimental.pallas import tpu as pltpu
from jax.sharding import PartitionSpec as P

BLOCK = 128
NX, NY, NZ = 4, 8, 8
STEPS = 4
CAP = 8
ROWS = 16
TOK = NX * ROWS
SLOTS = NX * CAP
COLD = 6
F32, BF16 = jnp.float32, jnp.bfloat16
ORDER = ((0, 7, 5, 2), (1, 3, 4, 6))
CORE_OF = tuple(0 if dy in ORDER[0] else 1 for dy in range(NY))
SEND_ORDER = (0, 1, 7, 6, 2, 3, 5, 4)
OWN = ORDER[0].index(0)
LAST = STEPS - 1
FAR_FIRST = (4, 3, 5, 2, 6, 1, 7)
MESH = pl.DeviceIdType.MESH


def dot(a, b):
    return jnp.dot(a, b, preferred_element_type=F32)


def dot_t(a, b):
    return lax.dot_general(a, b, (((0,), (0,)), ((), ())), preferred_element_type=F32)


def kernel(
    tok, hot_gate, hot_up, hot_down, cold_gate, cold_up, cold_down, hot_ids, cold_ids, mask,
    out,
    tokv, xbuf, wcg, wcu, wh, wd, maskv, hot_s, cold_s, hits, units, ptab, pmat, mz, sbuf, sown, rbuf, hbuf, obuf, oown, dbuf, ebuf, fbuf,
    xy_in, z_in, tok_sem, mask_sem, ids_sem, wl_sem, ws_sem, wr_sem,
    a1s, a1z, a1r, a2s, a2r, bs, br, cs, cr, d1s, d1r, d2s, d2z, d2r, d2zr,
):
    hot, cold = lax.axis_index("hot"), lax.axis_index("cold")
    z, k = lax.div(hot, 2), lax.rem(hot, 2)
    x, y = lax.div(cold, NY), lax.rem(cold, NY)
    feat = tok.shape[1]

    def dev(px, py, pz, pk):
        return {"hot": pz * 2 + pk, "cold": px * NY + py}

    def at_x(d):
        return lax.rem(x + (d % NX), NX)

    def at_y(d):
        return lax.rem(y + NY + d, NY)

    def at_z(d):
        return lax.rem(z + (d % NZ), NZ)

    def dy_of(s):
        return ORDER[0][s] + k * (ORDER[1][s] - ORDER[0][s])

    def remote(src, dst, send, recv, to):
        return pltpu.make_async_remote_copy(
            src_ref=src, dst_ref=dst, send_sem=send, recv_sem=recv, device_id=to, device_id_type=MESH
        )

    def parts_of(s):
        if s == LAST:
            return ((STEPS, slice(feat, 2 * feat)), (s, slice(0, feat)))
        return ((s, slice(0, 2 * feat)),)

    here = dev(x, y, z, k)
    sister = dev(x, y, z, 1 - k)
    cols = pl.ds(pl.multiple_of(k * feat, feat), feat)
    mine = pl.ds(pl.multiple_of(k * feat, feat), feat)

    tok_load = pltpu.make_async_copy(tok, tokv, tok_sem)
    tok_load.start()

    barrier = pltpu.get_barrier_semaphore()

    def greet(to):
        pl.semaphore_signal(barrier, inc=1, device_id=to, device_id_type=MESH)

    greet(sister)
    for d in range(1, NY):
        greet(dev(x, at_y(d), z, 1))
    for d in range(1, NX):
        greet(dev(at_x(d), y, z, 1))
    for d in FAR_FIRST:
        greet(dev(x, y, at_z(d), 0))

    mask_load = pltpu.make_async_copy(mask, maskv, mask_sem)
    hot_load = pltpu.make_async_copy(hot_ids, hot_s, ids_sem.at[0])
    cold_load = pltpu.make_async_copy(cold_ids, cold_s, ids_sem.at[1])
    pieces = (
        (cold_gate, wcg.at[mine, :]),
        (cold_up, wcu.at[mine, :]),
        (hot_gate, wh.at[mine, pl.ds(0, BLOCK)]),
        (hot_up, wh.at[mine, pl.ds(BLOCK, BLOCK)]),
        (cold_down, wd.at[pl.ds(0, COLD * BLOCK), cols]),
        (hot_down, wd.at[pl.ds(COLD * BLOCK, BLOCK), cols]),
    )
    local_w = [pltpu.make_async_copy(a, b, wl_sem.at[i]) for i, (a, b) in enumerate(pieces)]
    remote_w = [remote(a, b, ws_sem.at[i], wr_sem.at[i], sister) for i, (a, b) in enumerate(pieces)]
    tok_load.wait()

    @pl.when(k == 1)
    def _():
        pl.semaphore_wait(barrier, 2 * (NY - 1) + 2 * (NX - 1) + 1)
        pl.semaphore_signal(xy_in, inc=1, device_id=sister, device_id_type=MESH)

    @pl.when(k == 0)
    def _():
        pl.semaphore_wait(xy_in, 1)

    for dy in SEND_ORDER:
        core = CORE_OF[dy]
        s = ORDER[core].index(dy)
        spot = xbuf.at[s, pl.ds(0, ROWS), cols]
        if dy:
            remote(tokv, spot, a1s, a1r.at[s], dev(x, at_y(-dy), z, core)).start()
        else:

            @pl.when(k == 0)
            def _():
                pltpu.make_async_copy(tok, xbuf.at[OWN, pl.ds(0, ROWS), pl.ds(0, feat)], a1r.at[OWN]).start()

            @pl.when(k == 1)
            def _():
                remote(
                    tokv, xbuf.at[OWN, pl.ds(0, ROWS), pl.ds(feat, feat)], a1z, a1r.at[OWN], sister
                ).start()

    for copy in (mask_load, hot_load, cold_load):
        copy.start()
    for copy in local_w[:4] + remote_w[:4] + local_w[4:]:
        copy.start()

    def spread(s):
        head = xbuf.at[s, pl.ds(0, ROWS), :]
        remote(head, head, a2s.at[s], a1r.at[s], here).wait_recv()
        for dx in (2, 1, 3):
            remote(
                head, xbuf.at[s, pl.ds(dx * ROWS, ROWS), :], a2s.at[s], a2r.at[s], dev(at_x(-dx), y, z, k)
            ).start()

    def gate_up(s):
        rest = xbuf.at[s, pl.ds(ROWS, TOK - ROWS), :]
        remote(rest, rest, a2s.at[s], a2r.at[s], here).wait_recv()
        if s == 0:
            for i in range(4):
                local_w[i].wait()
                remote_w[i].wait_recv()
        rows = xbuf[s]
        picked = dot(pmat[s], rows).astype(BF16)
        gates, ups = dot(picked, wcg[...]), dot(picked, wcu[...])
        hots = dot(rows, wh[...])
        for j in range(NZ):
            if j < COLD:
                part = slice(j * BLOCK, (j + 1) * BLOCK)
                gate, up = gates[:, part], ups[:, part]
            else:
                part = slice((j - COLD) * SLOTS, (j - COLD + 1) * SLOTS)
                gate, up = hots[part, :BLOCK], hots[part, BLOCK:]
            sown[s, j, :, :BLOCK] = gate
            sown[s, j, :, BLOCK:] = up
            sbuf[s, j, :, :BLOCK] = gate.astype(BF16)
            sbuf[s, j, :, BLOCK:] = up.astype(BF16)
        if s == 0:

            @pl.when(k == 0)
            def _():
                pl.semaphore_wait(barrier, 2 * (NZ - 1) + 1)
                pl.semaphore_signal(z_in, inc=1, device_id=sister, device_id_type=MESH)

            @pl.when(k == 1)
            def _():
                pl.semaphore_wait(z_in, 1)

        for dz in FAR_FIRST:
            remote(
                sbuf.at[s, at_z(dz)], rbuf.at[s, dz - 1], bs.at[s], br.at[s], dev(x, y, at_z(dz), k)
            ).start()

    def share(s):
        remote(rbuf.at[s], rbuf.at[s], bs.at[s], br.at[s], here).wait_recv()
        terms = sown[s, z]
        for i in range(NZ - 1):
            terms = terms + rbuf[s, i].astype(F32)
        gate, up = terms[:, :BLOCK], terms[:, BLOCK:]
        hidden = gate / (1.0 + jnp.exp(-gate)) * up * mz[s]
        hbuf[s, z] = hidden.astype(BF16)
        for i in range(NZ - 1):
            to = i + jnp.where(z <= i, 1, 0)
            remote(hbuf.at[s, z], hbuf.at[s, z], cs.at[s], cr.at[s], dev(x, y, to, k)).start()

    spread(0)

    for copy in (mask_load, hot_load, cold_load):
        copy.wait()
    bits = maskv[...].astype(F32).astype(BF16)
    blocks = maskv.shape[0]
    block_no = lax.broadcasted_iota(jnp.int32, (blocks, BLOCK), 0)
    cold_sel = jnp.zeros((blocks, BLOCK), F32)
    for j in range(COLD):
        cold_sel = cold_sel + jnp.where(block_no == cold_s[cold * COLD + j], 1.0, 0.0)
    unit_id = jnp.where(z < COLD, cold_s[cold * COLD + jnp.minimum(z, COLD - 1)], hot_s[cold])
    unit_sel = jnp.where(block_no == unit_id, 1.0, 0.0)
    hits[...] = jnp.minimum(dot_t(bits, cold_sel.astype(BF16)), 1.0)
    units[...] = dot_t(bits, unit_sel.astype(BF16))

    def in_order(ref):
        starts = [(at_x(dx) * NY + at_y(dy_of(s))) * ROWS for s in range(STEPS) for dx in range(NX)]
        return jnp.concatenate([ref[pl.ds(pl.multiple_of(i, ROWS), ROWS), :] for i in starts], axis=0)

    hit, unit_bit = in_order(hits), in_order(units)
    total = STEPS * TOK
    row = lax.broadcasted_iota(jnp.int32, (total, total), 0)
    col = lax.broadcasted_iota(jnp.int32, (total, total), 1)
    earlier = (lax.div(row, ROWS) == lax.div(col, ROWS)) & (col < row)
    slot = dot(jnp.where(earlier, 1.0, 0.0).astype(BF16), hit.astype(BF16))
    row = lax.broadcasted_iota(jnp.int32, (total, BLOCK), 0)
    lane = lax.broadcasted_iota(jnp.int32, (total, BLOCK), 1)
    base = lax.rem(lax.div(row, ROWS), NX) * CAP
    chosen = jnp.where((slot + base.astype(F32) == lane.astype(F32)) & (hit > 0.5), 1.0, 0.0)
    for s in range(STEPS):
        step_rows = slice(s * TOK, (s + 1) * TOK)
        pick = chosen[step_rows]
        ptab[s] = pick.astype(BF16)
        turned = jnp.transpose(pick)[:SLOTS].astype(BF16)
        pmat[s] = turned
        tokens_bit = unit_bit[step_rows]
        slot_bit = dot(turned, tokens_bit.astype(BF16))
        half_bit = jnp.where(z == COLD, tokens_bit[:SLOTS], tokens_bit[SLOTS:])
        mz[s] = jnp.where(z < COLD, slot_bit, half_bit)

    spread(1)
    gate_up(0)
    spread(3)
    spread(2)
    for copy in remote_w[4:]:
        copy.start()
    def down(s):
        most = hbuf.at[s, pl.ds(0, NZ - 1)]
        remote(most, most, cs.at[s], cr.at[s], here).wait_recv()
        if s == 0:
            for i in (4, 5):
                local_w[i].wait()
                remote_w[i].wait_recv()
        colds = jnp.concatenate([hbuf[s, j] for j in range(COLD)], axis=1)
        placed = dot(ptab[s][:, :SLOTS], colds).astype(BF16)
        hots = jnp.concatenate([hbuf[s, COLD], hbuf[s, COLD + 1]], axis=0)
        for index, part in parts_of(s):
            result = dot(placed, wd[: COLD * BLOCK, part]) + dot(hots, wd[COLD * BLOCK :, part])
            oown[s, :, part] = result[:ROWS]
            obuf[s, :, part] = result.astype(BF16)
            for dx in (2, 1, 3):
                remote(
                    obuf.at[s, pl.ds(dx * ROWS, ROWS), part], dbuf.at[s, dx - 1, :, part], d1s.at[index],
                    d1r.at[index], dev(at_x(dx), y, z, k),
                ).start()

    def collect(s):
        dy = dy_of(s)
        for index, part in parts_of(s):
            sums = dbuf.at[s, :, :, part]
            remote(sums, sums, d1s.at[index], d1r.at[index], here).wait_recv()
            terms = oown[s, :, part]
            for i in range(NX - 1):
                terms = terms + dbuf[s, i, :, part].astype(F32)
            for f in range(2):
                if index == s and s == LAST and f == 1:
                    continue
                if index != s and f == 0:
                    continue
                piece = terms[:, f * feat : (f + 1) * feat] if terms.shape[1] > feat else terms
                ebuf[s, f] = piece.astype(BF16)
                if s == LAST:
                    remote(ebuf.at[s, f], fbuf.at[dy], d2s.at[s], d2r, dev(x, at_y(dy), z, f)).start()
        if s == LAST:
            return

        def to_owners():
            for f in range(2):
                remote(
                    ebuf.at[s, f], fbuf.at[dy], d2s.at[s], d2r, dev(x, at_y(dy), z, f)
                ).start()

        if s != OWN:
            to_owners()
        else:
            pl.when(k == 1)(to_owners)

            @pl.when(k == 0)
            def _():
                remote(ebuf.at[OWN, 1], fbuf.at[0], d2z, d2zr, sister).start()
                fbuf[0] = ebuf[OWN, 0]

    gate_up(1)
    share(0)
    gate_up(2)
    share(1)
    gate_up(3)
    share(2)
    down(0)
    share(3)
    down(1)
    collect(0)
    down(2)
    down(3)
    collect(1)
    collect(2)
    collect(3)

    remote(fbuf.at[pl.ds(1, NY - 1)], fbuf.at[pl.ds(1, NY - 1)], a1s, d2r, here).wait_recv()

    @pl.when(k == 1)
    def _():
        remote(fbuf.at[0], fbuf.at[0], d2z, d2zr, here).wait_recv()

    answer = fbuf[0].astype(F32)
    for dy in range(1, NY):
        answer = answer + fbuf[dy].astype(F32)
    out[...] = answer.astype(BF16)

    seven = fbuf.at[pl.ds(1, NY - 1)]
    remote(seven, seven, a1s, d2r, here).wait_send()
    for copy in remote_w:
        copy.wait_send()
    for s in range(STEPS):
        rest = xbuf.at[s, pl.ds(ROWS, TOK - ROWS), :]
        remote(rest, rest, a2s.at[s], a2r.at[s], here).wait_send()
        remote(rbuf.at[s], rbuf.at[s], bs.at[s], br.at[s], here).wait_send()
        most = hbuf.at[s, pl.ds(0, NZ - 1)]
        remote(most, most, cs.at[s], cr.at[s], here).wait_send()
        for index, part in parts_of(s):
            sums = dbuf.at[s, :, :, part]
            remote(sums, sums, d1s.at[index], d1r.at[index], here).wait_send()
        if s != OWN:
            remote(ebuf.at[s], ebuf.at[s], d2s.at[s], d2r, here).wait_send()

    @pl.when(k == 1)
    def _():
        remote(ebuf.at[OWN], ebuf.at[OWN], d2s.at[OWN], d2r, here).wait_send()
        remote(tokv, tokv, a1z, a1r.at[OWN], here).wait_send()

    @pl.when(k == 0)
    def _():
        remote(ebuf.at[OWN, 1], ebuf.at[OWN, 1], d2z, d2zr, here).wait_send()


def body(*args):
    rows, feat = args[0].shape
    hbm = pl.BlockSpec(memory_space=pl.ANY)
    args = (*args[:9], args[9].T)
    blocks, tokens = args[9].shape
    dma = pltpu.SemaphoreType.DMA
    args = tuple(pltpu.with_memory_space_constraint(a, pltpu.HBM) for a in args)
    return pl.pallas_call(
        kernel,
        out_shape=jax.ShapeDtypeStruct((rows, feat), BF16),
        in_specs=[hbm] * 10,
        out_specs=pl.BlockSpec(memory_space=pltpu.VMEM),
        scratch_shapes=[
            pltpu.VMEM((ROWS, feat), BF16),
            pltpu.VMEM((STEPS, TOK, 2 * feat), BF16),
            pltpu.VMEM((2 * feat, COLD * BLOCK), BF16),
            pltpu.VMEM((2 * feat, COLD * BLOCK), BF16),
            pltpu.VMEM((2 * feat, 2 * BLOCK), BF16),
            pltpu.VMEM(((COLD + 1) * BLOCK, 2 * feat), BF16),
            pltpu.VMEM((blocks, tokens), jnp.int32),
            pltpu.SMEM(args[7].shape, jnp.int32),
            pltpu.SMEM(args[8].shape, jnp.int32),
            pltpu.VMEM((tokens, BLOCK), F32),
            pltpu.VMEM((tokens, BLOCK), F32),
            pltpu.VMEM((STEPS, TOK, BLOCK), BF16),
            pltpu.VMEM((STEPS, SLOTS, TOK), BF16),
            pltpu.VMEM((STEPS, SLOTS, BLOCK), F32),
            pltpu.VMEM((STEPS, NZ, SLOTS, 2 * BLOCK), BF16),
            pltpu.VMEM((STEPS, NZ, SLOTS, 2 * BLOCK), F32),
            pltpu.VMEM((STEPS, NZ - 1, SLOTS, 2 * BLOCK), BF16),
            pltpu.VMEM((STEPS, NZ, SLOTS, BLOCK), BF16),
            pltpu.VMEM((STEPS, TOK, 2 * feat), BF16),
            pltpu.VMEM((STEPS, ROWS, 2 * feat), F32),
            pltpu.VMEM((STEPS, NX - 1, ROWS, 2 * feat), BF16),
            pltpu.VMEM((STEPS, 2, ROWS, feat), BF16),
            pltpu.VMEM((NY, ROWS, feat), BF16),
            pltpu.SemaphoreType.REGULAR, pltpu.SemaphoreType.REGULAR,
            dma, dma, dma((2,)), dma((6,)), dma((6,)), dma((6,)),
            dma, dma, dma((STEPS,)), dma((STEPS,)), dma((STEPS,)),
            dma((STEPS,)), dma((STEPS,)), dma((STEPS,)), dma((STEPS,)),
            dma((STEPS + 1,)), dma((STEPS + 1,)), dma((STEPS,)), dma, dma, dma,
        ],
        compiler_params=pltpu.CompilerParams(collective_id=0, has_side_effects=True, vmem_limit_bytes=32 * 2**20),
    )(*args)


def solution(mesh):
    return jax.shard_map(
        body,
        mesh=mesh,
        in_specs=(
            P("cold", "hot"),
            P("hot", "cold"),
            P("hot", "cold"),
            P("cold", "hot"),
            P("hot", "cold"),
            P("hot", "cold"),
            P("cold", "hot"),
            P(),
            P(),
            P(),
        ),
        out_specs=P("cold", "hot"),
        check_vma=False,
    )
```
